32 devices in a mesh: row: 4 (over y, core), col: 8 (over z, x).
Axes of the slice: x: 2, y: 2, z: 4, core: 2. Of those that a mesh axis runs over, the one named last changes fastest.
Arguments:
- text_features: bfloat16 [5, 1024, 3584], P(None, ('row', 'col')), may hold values from -18 to 18
- vision_features: bfloat16 [6, 1024, 1024], P(None, ('row', 'col')), may hold values from -18 to 18
Outputs:
- stimulus_terms: float32 [1024, 30], P(('row', 'col'))
- cka: float32 [5, 6], replicated
The draws below stay inside these ranges and needn't reach their ends.
All inputs are finite; a program needn't handle non-finite values.
Results may differ from the reference program's by a relative error of at most 0.0003.
Values may be sent and summed in bfloat16 or wider, within the bound.
No kernel may reach another device: no remote copies, remote signals or barrier semaphores. Data moves between devices by JAX's collectives and lax.ppermute only.
A program may use at most 192 MiB of HBM per device.

```python
import math
import jax
import jax.numpy as jnp
from jax import lax

DA = 3584
DB = 1024
LA = 5
LB = 6
STIMULI = 1024


def shared_latent(key):
    key_latent = jax.random.fold_in(key, 21)
    key_scale = jax.random.fold_in(key, 22)
    latent = jax.random.truncated_normal(key_latent, -4.0, 4.0, (STIMULI, DB // 4), jnp.float32)
    top_scale = math.log(3.0)
    scales = jnp.exp(jax.random.uniform(key_scale, (STIMULI, 1), jnp.float32, 0.0, top_scale))
    return latent * scales


def feature_draw(key, modality, layers, width):
    latent = shared_latent(key)
    own_key = jax.random.fold_in(key, modality)
    key_offset = jax.random.fold_in(own_key, 11)
    key_noise = jax.random.fold_in(own_key, 12)
    key_project = jax.random.fold_in(own_key, 13)
    key_strength = jax.random.fold_in(own_key, 14)
    offsets = jax.random.uniform(key_offset, (layers, 1, width), jnp.float32, -2.0, 2.0)
    noise = jax.random.truncated_normal(key_noise, -4.0, 4.0, (layers, STIMULI, width), jnp.float32)
    projection = jax.random.truncated_normal(key_project, -4.0, 4.0, (layers, DB // 4, width), jnp.float32) * (DB // 4) ** (-0.5)
    strength = jax.random.uniform(key_strength, (layers, 1, 1), jnp.float32, 0.5, 0.9)
    signal = jnp.einsum('sr,lrw->lsw', latent, projection, precision=lax.Precision.HIGHEST) * strength
    values = jnp.clip(noise + signal, -16.0, 16.0) + offsets
    return values.astype(jnp.bfloat16)


def draw_text_features(key, part):
    return feature_draw(key, 1, LA, DA)


def draw_vision_features(key, part):
    return feature_draw(key, 2, LB, DB)


def setup_inputs(seed: int = 0) -> dict:
    arg_keys = jax.random.split(jax.random.key(seed), 3)
    return {
        "text_features": draw_text_features(jax.random.fold_in(arg_keys[2], 71), 0),
        "vision_features": draw_vision_features(jax.random.fold_in(arg_keys[2], 71), 0),
    }


def center_features(features):
    values = features.astype(jnp.float32)
    mean_values = lax.optimization_barrier(jnp.sum(values, axis=1, keepdims=True)) / values.shape[1]
    return (values - mean_values).astype(jnp.bfloat16)

def reference(text_features, vision_features):
    text_centered = center_features(text_features)
    vision_centered = center_features(vision_features).astype(jnp.float32)
    vision_grams = jnp.einsum('lsd,ltd->lst', vision_centered, vision_centered, precision=lax.Precision.HIGHEST)
    vision_self = lax.optimization_barrier(jnp.sum(vision_grams * vision_grams, axis=(1, 2)))

    def per_text(layer_feats):
        gram = jnp.dot(layer_feats, layer_feats.T, preferred_element_type=jnp.float32)
        share = jnp.einsum('st,mst->sm', gram, vision_grams, precision=lax.Precision.HIGHEST)
        return (share, jnp.sum(gram * gram))
    row_share, text_self = lax.map(per_text, text_centered)
    scale = 1.0 / jnp.sqrt(text_self[:, None] * vision_self[None, :])
    cross = lax.optimization_barrier(jnp.sum(row_share, axis=1))
    cka = cross * scale
    terms = jnp.transpose(row_share, (1, 0, 2)) * scale[None] * STIMULI
    return (terms.reshape(STIMULI, LA * LB), cka)
```

```python
import math

import jax
import jax.numpy as jnp
import numpy as np
from jax import lax
from jax.experimental import pallas as pl
from jax.experimental.pallas import tpu as pltpu
from jax.sharding import PartitionSpec as P


AXES = ("row", "col")
NT = (((1,), (1,)), ((), ()))


class Grid:
    def __init__(self, mesh):
        devices = mesh.devices
        rows, cols = devices.shape
        flat = list(devices.flat)
        places = [getattr(d, "coords", None) for d in flat]
        if all(p is not None for p in places):
            at = [(*p[:3], getattr(d, "core_on_chip", 0)) for p, d in zip(places, flat)]
        else:
            at = [(0, r, c, 0) for r in range(rows) for c in range(cols)]
        levels = [sorted({a[k] for a in at}) for k in range(4)]
        self.at = [tuple(levels[k].index(a[k]) for k in range(4)) for a in at]
        self.size = tuple(len(v) for v in levels)
        self.index = {a: i for i, a in enumerate(self.at)}
        if len(self.index) != len(flat) or len(flat) != math.prod(self.size):
            self.at = [(0, r, c, 0) for r in range(rows) for c in range(cols)]
            self.size = (1, rows, cols, 1)
            self.index = {a: i for i, a in enumerate(self.at)}

    def moved(self, i, shift):
        return self.index[tuple((p + s) % n for p, s, n in zip(self.at[i], shift, self.size))]

    def pairs(self, shift, senders=None):
        return [(i, self.moved(i, shift)) for i in range(len(self.at)) if senders is None or senders(self.at[i])]


def pack_kernel(kt, kv, width, start, text_ref, vision_ref, packed_ref, sums_ref):
    for k in range(kt * text_ref.shape[0], start):
        packed_ref[k] = jnp.zeros(packed_ref.shape[1:], packed_ref.dtype)
        sums_ref[pl.ds(k, 1), :] = jnp.zeros((1, width), jnp.float32)
    for ref, per, first in ((text_ref, kt, 0), (vision_ref, kv, start)):
        for layer in range(ref.shape[0]):
            for k in range(per):
                values = ref[layer, :, k * width : (k + 1) * width]
                packed_ref[first + layer * per + k] = values
                sums_ref[pl.ds(first + layer * per + k, 1), :] = jnp.sum(
                    values.astype(jnp.float32), axis=0, keepdims=True
                )


def pack(text, vision, kt, kv, width, start):
    chunks = start + kv * vision.shape[0]
    rows = text.shape[1]
    return pl.pallas_call(
        lambda *refs: pack_kernel(kt, kv, width, start, *refs),
        out_shape=(
            jax.ShapeDtypeStruct((chunks, rows, width), text.dtype),
            jax.ShapeDtypeStruct((chunks, width), jnp.float32),
        ),
        name="pack",
    )(text, vision)


def tiles_kernel(
    la, lb, kt, kv, rows, na, nb, ndest, count,
    dest_ref, weight_ref, *refs,
):
    ins, payload_ref, scratch = refs[: 2 * (na + nb) + 2], refs[2 * (na + nb) + 2], refs[2 * (na + nb) + 3 :]
    ac, bc, k1, k2, g1, g2, cols_ref, rows_ref = scratch
    step = pl.program_id(0)
    width = ins[0].shape[-1]

    def layer(blocks, mean_ref, per, out1, out2, i):
        for k in range(per):
            mean = mean_ref[0, k : k + 1, :] * (1.0 / count)
            for j, ref in enumerate(blocks):
                centered = (ref[k].astype(jnp.float32) - mean).astype(jnp.bfloat16)
                if j < na:
                    ac[pl.ds(j * rows, rows), pl.ds(k * width, width)] = centered
                if j == 0:
                    bc[pl.ds(nb * rows, rows), pl.ds(k * width, width)] = centered
                if j >= na:
                    bc[pl.ds((j - na) * rows, rows), pl.ds(k * width, width)] = centered
        a = ac[:, pl.ds(0, per * width)]
        b = bc[:, pl.ds(0, per * width)]
        out1[i] = lax.dot_general(a, b, NT, preferred_element_type=jnp.float32)
        out2[i] = lax.dot_general(b[: nb * rows], a, NT, preferred_element_type=jnp.float32)

    @pl.when(step < la)
    def _():
        layer(ins[: na + nb], ins[-2], kt, k1, k2, step)

    @pl.when(step < lb)
    def _():
        layer(ins[na + nb : 2 * (na + nb)], ins[-1], kv, g1, g2, step)

    @pl.when(step == max(la, lb) - 1)
    def _():
        pairs = la * lb
        nbr = (nb + 1) * rows
        cols_ref[...] = jnp.zeros_like(cols_ref)
        rows_ref[...] = jnp.zeros_like(rows_ref)
        lane = lax.broadcasted_iota(jnp.int32, (1, 128), 1)
        wlast = weight_ref[0]
        block = lane // rows
        cell = jnp.where(block < nb - 1, 2.0, jnp.where(block == nb - 1, 2.0 * wlast, 1.0))
        cell = jnp.where(block <= nb, cell, 0.0)
        for a in range(la):
            for b in range(lb):
                p = a * lb + b
                cols_ref[p : p + 1, 0:nbr] = jnp.sum(k1[a] * g1[b], axis=0, keepdims=True)
                prod = k2[a] * g2[b]
                rows_ref[p : p + 1, :] = jnp.sum(prod[: (nb - 1) * rows], axis=0, keepdims=True) + wlast * jnp.sum(
                    prod[(nb - 1) * rows :], axis=0, keepdims=True
                )
        for a in range(la):
            cols_ref[pairs + a : pairs + a + 1, 0:nbr] = jnp.sum(k1[a] * k1[a], axis=0, keepdims=True)
        for b in range(lb):
            cols_ref[pairs + la + b : pairs + la + b + 1, 0:nbr] = jnp.sum(g1[b] * g1[b], axis=0, keepdims=True)
        totals = jnp.sum((cols_ref[...] * cell).T, axis=0, keepdims=True)
        q_count = 128 // rows
        sub = lax.broadcasted_iota(jnp.int32, (8, 128), 0)
        lane8 = lax.broadcasted_iota(jnp.int32, (8, 128), 1)
        spot = (lane8 // rows) * 8 + sub
        own = lane8 % rows
        spread = jnp.broadcast_to(totals, (8, 128))

        def shifted(x, by):
            by %= 128
            return pltpu.roll(x, by, 1) if by else x

        base = jnp.zeros((8, 128), jnp.float32)
        q_cross, q_self = pairs // 8, (pairs + 1) // 8
        base = jnp.where((spot == pairs) & (own < pairs), shifted(spread, q_cross * rows), base)
        base = jnp.where((spot == pairs + 1) & (own < la + lb), shifted(spread, q_self * rows - pairs), base)
        for d in range(ndest):
            payload_ref[d] = base
        for j in range(na + nb):
            tile = base
            for q in range(q_count):
                if j < na:
                    c0 = j * rows
                    part = shifted(rows_ref[8 * q : 8 * q + 8, c0 // 128 * 128 : c0 // 128 * 128 + 128], q * rows - c0 % 128)
                    if j == 0:
                        part = part + shifted(cols_ref[8 * q : 8 * q + 8, :], (q - nb) * rows)
                else:
                    part = shifted(cols_ref[8 * q : 8 * q + 8, :], (q - (j - na)) * rows)
                    if j == na + nb - 1:
                        part = part * wlast
                tile = jnp.where((lane8 // rows == q) & (spot < pairs), part, tile)
            payload_ref[dest_ref[j]] = tile


def tiles(a_blocks, b_blocks, totals, dest, weight, la, lb, kt, kv, start, count, ndest):
    na, nb = len(a_blocks), len(b_blocks)
    blocks = [*a_blocks, *b_blocks]
    rows, width = blocks[0].shape[1:]
    assert (nb + 1) * rows <= 128 and 128 % rows == 0
    assert 8 * (128 // rows) >= la * lb + 2 and la * lb + la + lb <= 128 and la * lb <= rows and nb >= 1
    steps = max(la, lb)
    smem = pl.BlockSpec(memory_space=pltpu.SMEM)
    text_spec = pl.BlockSpec((kt, rows, width), lambda i: (jnp.minimum(i, la - 1), 0, 0))
    vision_spec = pl.BlockSpec((kv, rows, width), lambda i: (start // kv + jnp.minimum(i, lb - 1), 0, 0))
    mean_t = totals[: la * kt].reshape(la, kt, width)
    mean_v = totals[start:].reshape(lb, kv, width)
    return pl.pallas_call(
        lambda *refs: tiles_kernel(la, lb, kt, kv, rows, na, nb, ndest, count, *refs),
        grid=(steps,),
        in_specs=[smem, smem]
        + [text_spec] * (na + nb)
        + [vision_spec] * (na + nb)
        + [
            pl.BlockSpec((1, kt, width), lambda i: (jnp.minimum(i, la - 1), 0, 0)),
            pl.BlockSpec((1, kv, width), lambda i: (jnp.minimum(i, lb - 1), 0, 0)),
        ],
        out_specs=pl.BlockSpec((ndest, 8, 128), lambda i: (0, 0, 0)),
        out_shape=jax.ShapeDtypeStruct((ndest, 8, 128), jnp.float32),
        scratch_shapes=[
            pltpu.VMEM((na * rows, max(kt, kv) * width), jnp.bfloat16),
            pltpu.VMEM(((nb + 1) * rows, max(kt, kv) * width), jnp.bfloat16),
            pltpu.VMEM((la, na * rows, (nb + 1) * rows), jnp.float32),
            pltpu.VMEM((la, nb * rows, na * rows), jnp.float32),
            pltpu.VMEM((lb, na * rows, (nb + 1) * rows), jnp.float32),
            pltpu.VMEM((lb, nb * rows, na * rows), jnp.float32),
            pltpu.VMEM((128, 128), jnp.float32),
            pltpu.VMEM((8 * (128 // rows), max(128, na * rows)), jnp.float32),
        ],
        compiler_params=pltpu.CompilerParams(vmem_limit_bytes=56 * 1024 * 1024),
        name="tiles",
    )(dest, weight, *blocks, *blocks, mean_t, mean_v)


def finish_kernel(la, lb, rows, count, in_ref, terms_ref, cka_ref):
    pairs = la * lb
    total = jnp.sum(in_ref[...], axis=0)
    spots = jnp.concatenate([total[:, q * rows : (q + 1) * rows] for q in range(128 // rows)], axis=0)
    cross = spots[pairs : pairs + 1, :]
    selves = jnp.broadcast_to(spots[pairs + 1 : pairs + 2, :], (rows, rows)).T
    sub = lax.broadcasted_iota(jnp.int32, (rows, rows), 0)
    lane = lax.broadcasted_iota(jnp.int32, (rows, rows), 1)
    text = jnp.sum(jnp.where(sub == lane // lb, selves, 0.0), axis=0, keepdims=True)
    vision = jnp.sum(jnp.where(sub == la + lane % lb, selves, 0.0), axis=0, keepdims=True)
    inside = lax.broadcasted_iota(jnp.int32, (1, rows), 1) < pairs
    scale = 1.0 / jnp.sqrt(jnp.where(inside, text * vision, 1.0))
    terms = spots.T * (scale * count) if spots.shape[0] == rows else spots.T[:, :rows] * (scale * count)
    terms_ref[...] = terms[:, :pairs]
    cka = cross * scale
    for a in range(la):
        cka_ref[a : a + 1, :] = cka[:, a * lb : (a + 1) * lb]


def finish(received, la, lb, rows, count):
    return pl.pallas_call(
        lambda *refs: finish_kernel(la, lb, rows, count, *refs),
        out_shape=(
            jax.ShapeDtypeStruct((rows, la * lb), jnp.float32),
            jax.ShapeDtypeStruct((la, lb), jnp.float32),
        ),
        name="finish",
    )(received)


def solution(mesh):
    grid = Grid(mesh)
    nx, ny, nz, nc = grid.size
    ndev = len(grid.at)

    def send(value, shift, senders=None):
        return lax.ppermute(value, AXES, grid.pairs(shift, senders))

    def half_sender(place):
        z = place[2]
        return (z < nz // 2) == ((z % (nz // 2)) % 2 == 0)

    def body(text, vision):
        la, rows, da = text.shape
        lb, _, db = vision.shape
        count = rows * ndev
        width = math.gcd(da, db)
        kt, kv = da // width, db // width
        start = -(-la * kt // kv) * kv
        me = lax.axis_index(AXES)
        own, sums = pack(text, vision, kt, kv, width, start)
        chunks = own.shape[0]

        b_blocks, b_shifts = [], []
        full_shifts = range(1, (nz + 1) // 2)
        for d in full_shifts:
            b_blocks.append(send(own, (0, 0, d, 0)))
            b_shifts.append((0, 0, d, 0))

        for d in range(1, nc):
            sums = sums + send(sums, (0, 0, 0, d))
        part = sums
        for d in range(1, nx):
            sums = sums + send(part, (d, 0, 0, 0))
        part = sums
        for d in range(1, ny):
            sums = sums + send(part, (0, d, 0, 0))
        part = sums
        for d in range(1, nz):
            sums = sums + send(part, (0, 0, d, 0))

        plane = {(0, 0): own}
        for d in range(1, nx):
            plane[d, 0] = send(own, (d, 0, 0, 0))
        for d in range(1, ny):
            plane[0, d] = send(own, (0, d, 0, 0))
        half = chunks // 2
        for dx in range(1, nx):
            for dy in range(1, ny):
                first = send(plane[dx, 0][:half], (0, dy, 0, 0))
                second = send(plane[0, dy][half:], (dx, 0, 0, 0))
                plane[dx, dy] = jnp.concatenate([first, second], axis=0)
        a_blocks, a_shifts = [], []
        for (dx, dy), block in plane.items():
            a_blocks.append(block)
            a_shifts.append((dx, dy, 0, 0))
            for dc in range(1, nc):
                a_blocks.append(send(block, (0, 0, 0, dc)))
                a_shifts.append((dx, dy, 0, dc))

        weight = np.zeros((ndev,), np.float32)
        if nz % 2 == 0:
            b_blocks.append(send(own, (0, 0, nz // 2, 0), half_sender))
            b_shifts.append((0, 0, nz // 2, 0))
            for i in range(ndev):
                if half_sender(grid.at[i]):
                    weight[grid.moved(i, (0, 0, nz // 2, 0))] = 1.0
        else:
            weight[:] = 1.0
        shifts = a_shifts + b_shifts
        table = np.array(
            [[grid.moved(i, tuple(-s for s in shift)) for shift in shifts] for i in range(ndev)], np.int32
        )
        dest = lax.dynamic_index_in_dim(jnp.asarray(table), me, 0, keepdims=False)
        w = lax.dynamic_slice_in_dim(jnp.asarray(weight), me, 1)
        payload = tiles(a_blocks, b_blocks, sums, dest, w, la, lb, kt, kv, start, count, ndev)
        received = lax.all_to_all(payload, AXES, 0, 0, tiled=True)
        return finish(received, la, lb, rows, count)

    spec = P(None, AXES, None)
    return jax.shard_map(body, mesh=mesh, in_specs=(spec, spec), out_specs=(P(AXES, None), P()), check_vma=False)
```

```python
import math

import jax
import jax.numpy as jnp
import numpy as np
from jax import lax
from jax.experimental import pallas as pl
from jax.experimental.pallas import tpu as pltpu
from jax.sharding import PartitionSpec as P


AXES = ("row", "col")
NT = (((1,), (1,)), ((), ()))


class Grid:
    def __init__(self, mesh):
        devices = mesh.devices
        rows, cols = devices.shape
        flat = list(devices.flat)
        places = [getattr(d, "coords", None) for d in flat]
        if all(p is not None for p in places):
            at = [(*p[:3], getattr(d, "core_on_chip", 0)) for p, d in zip(places, flat)]
        else:
            at = [(0, r, c, 0) for r in range(rows) for c in range(cols)]
        levels = [sorted({a[k] for a in at}) for k in range(4)]
        self.at = [tuple(levels[k].index(a[k]) for k in range(4)) for a in at]
        self.size = tuple(len(v) for v in levels)
        self.index = {a: i for i, a in enumerate(self.at)}
        if len(self.index) != len(flat) or len(flat) != math.prod(self.size):
            self.at = [(0, r, c, 0) for r in range(rows) for c in range(cols)]
            self.size = (1, rows, cols, 1)
            self.index = {a: i for i, a in enumerate(self.at)}

    def moved(self, i, shift):
        return self.index[tuple((p + s) % n for p, s, n in zip(self.at[i], shift, self.size))]

    def pairs(self, shift, senders=None):
        return [(i, self.moved(i, shift)) for i in range(len(self.at)) if senders is None or senders(self.at[i])]


def pack_kernel(kt, kv, width, start, text_ref, vision_ref, packed_ref, sums_ref):
    for k in range(kt * text_ref.shape[0], start):
        packed_ref[k] = jnp.zeros(packed_ref.shape[1:], packed_ref.dtype)
        sums_ref[pl.ds(k, 1), :] = jnp.zeros((1, width), jnp.float32)
    for ref, per, first in ((text_ref, kt, 0), (vision_ref, kv, start)):
        for layer in range(ref.shape[0]):
            for k in range(per):
                values = ref[layer, :, k * width : (k + 1) * width]
                packed_ref[first + layer * per + k] = values
                sums_ref[pl.ds(first + layer * per + k, 1), :] = jnp.sum(
                    values.astype(jnp.float32), axis=0, keepdims=True
                )


def pack(text, vision, kt, kv, width, start):
    chunks = start + kv * vision.shape[0]
    rows = text.shape[1]
    return pl.pallas_call(
        lambda *refs: pack_kernel(kt, kv, width, start, *refs),
        out_shape=(
            jax.ShapeDtypeStruct((chunks, rows, width), text.dtype),
            jax.ShapeDtypeStruct((chunks, width), jnp.float32),
        ),
        name="pack",
    )(text, vision)


def centered_rows(refs, mean_ref, first, per, count, out_ref, layer):
    rows, width = refs[0].shape[1:]
    for k in range(per):
        mean = mean_ref[pl.ds(first + k, 1), :] * (1.0 / count)
        for j, ref in enumerate(refs):
            out_ref[layer, pl.ds(j * rows, rows), pl.ds(k * width, width)] = (
                ref[k].astype(jnp.float32) - mean
            ).astype(jnp.bfloat16)


def add_products(la, lb, ks, gs, low, rows_ref, cols_ref):
    pairs = la * lb
    for a in range(la):
        for b in range(lb):
            prod = ks[a] * gs[b]
            rows_ref[pl.ds(a * lb + b, 1), :] = jnp.sum(prod[low:], axis=0, keepdims=True)
            cols_ref[:, pl.ds(a * lb + b, 1)] = jnp.sum(prod, axis=1, keepdims=True)
    for n, refs in ((pairs, ks), (pairs + la, gs)):
        for i in range(refs.shape[0]):
            cols_ref[:, pl.ds(n + i, 1)] = jnp.sum(refs[i] * refs[i], axis=1, keepdims=True)


def region_kernel(geo, na, nb, mean_ref, *refs):
    la, lb, kt, kv, start, rows, count = geo
    n = na + nb
    text, vision = refs[:n], refs[n : 2 * n]
    text_out, vision_out, rows_out, cols_out, bt, bv, ks, gs = refs[2 * n :]
    step = pl.program_id(0)

    def layer(blocks, per, first, out, bc, store):
        centered_rows(blocks[:na], mean_ref, first, per, count, out, 0)
        centered_rows(blocks[na:], mean_ref, first, per, count, bc, 0)
        store[step] = lax.dot_general(bc[0], out[0], NT, preferred_element_type=jnp.float32)

    @pl.when(step < la)
    def _():
        layer(text, kt, step * kt, text_out, bt, ks)

    @pl.when(step < lb)
    def _():
        layer(vision, kv, start + step * kv, vision_out, bv, gs)

    @pl.when(step == max(la, lb) - 1)
    def _():
        rows_out[...] = jnp.zeros_like(rows_out)
        cols_out[...] = jnp.zeros_like(cols_out)
        add_products(la, lb, ks, gs, rows, rows_out, cols_out)


def layer_specs(geo, n):
    la, lb, kt, kv, start, rows, _ = geo

    def of(width):
        text = pl.BlockSpec((kt, rows, width), lambda i: (jnp.minimum(i, la - 1), 0, 0))
        vision = pl.BlockSpec((kv, rows, width), lambda i: (start // kv + jnp.minimum(i, lb - 1), 0, 0))
        return [text] * n + [vision] * n

    return of


def region(geo, a_blocks, b_blocks, totals):
    la, lb, kt, kv, _, rows, _ = geo
    na, nb = len(a_blocks), len(b_blocks)
    width = totals.shape[-1]
    blocks = [*a_blocks, *b_blocks]
    return pl.pallas_call(
        lambda *refs: region_kernel(geo, na, nb, *refs),
        grid=(max(la, lb),),
        in_specs=[pl.BlockSpec(totals.shape, lambda i: (0, 0))] + layer_specs(geo, na + nb)(width),
        out_specs=[
            pl.BlockSpec((1, na * rows, kt * width), lambda i: (jnp.minimum(i, la - 1), 0, 0)),
            pl.BlockSpec((1, na * rows, kv * width), lambda i: (jnp.minimum(i, lb - 1), 0, 0)),
            pl.BlockSpec((8 * (128 // rows), na * rows), lambda i: (0, 0)),
            pl.BlockSpec((nb * rows, 128), lambda i: (0, 0)),
        ],
        out_shape=(
            jax.ShapeDtypeStruct((la, na * rows, kt * width), jnp.bfloat16),
            jax.ShapeDtypeStruct((lb, na * rows, kv * width), jnp.bfloat16),
            jax.ShapeDtypeStruct((8 * (128 // rows), na * rows), jnp.float32),
            jax.ShapeDtypeStruct((nb * rows, 128), jnp.float32),
        ),
        scratch_shapes=[
            pltpu.VMEM((1, nb * rows, kt * width), jnp.bfloat16),
            pltpu.VMEM((1, nb * rows, kv * width), jnp.bfloat16),
            pltpu.VMEM((la, nb * rows, na * rows), jnp.float32),
            pltpu.VMEM((lb, nb * rows, na * rows), jnp.float32),
        ],
        cost_estimate=pl.CostEstimate(flops=4_000_000_000, bytes_accessed=16_000_000, transcendentals=0),
        compiler_params=pltpu.CompilerParams(vmem_limit_bytes=56 * 1024 * 1024),
    )(totals, *blocks, *blocks)


def last_kernel(geo, parts, nb, ndest, dest_ref, weight_ref, mean_ref, *refs):
    la, lb, kt, kv, start, rows, count = geo
    npart = len(parts)
    last_text, last_vision = refs[0], refs[1]
    texts, visions = refs[2 : 2 + npart], refs[2 + npart : 2 + 2 * npart]
    part_rows = refs[2 + 2 * npart : 2 + 3 * npart]
    part_cols = refs[2 + 3 * npart : 2 + 4 * npart]
    payload_ref = refs[2 + 4 * npart]
    ct, cv, ks, gs, rows_ref, cols_ref, all_ref = refs[3 + 4 * npart :]
    step = pl.program_id(0)

    def layer(block, per, first, centered, others, store):
        centered_rows([block], mean_ref, first, per, count, centered, 0)
        at = 0
        for other in others:
            size = other.shape[1]
            store[step, :, at : at + size] = lax.dot_general(
                centered[0], other[0], NT, preferred_element_type=jnp.float32
            )
            at += size

    @pl.when(step < la)
    def _():
        layer(last_text, kt, step * kt, ct, texts, ks)

    @pl.when(step < lb)
    def _():
        layer(last_vision, kv, start + step * kv, cv, visions, gs)

    @pl.when(step == max(la, lb) - 1)
    def _():
        pairs = la * lb
        wlast = weight_ref[0]
        rows_ref[...] = jnp.zeros_like(rows_ref)
        cols_ref[...] = jnp.zeros_like(cols_ref)
        add_products(la, lb, ks, gs, 0, rows_ref, cols_ref)
        at = 0
        for ref in part_rows:
            size = ref.shape[1]
            rows_ref[:, at : at + size] = ref[...] + wlast * rows_ref[:, at : at + size]
            at += size
        early = part_cols[0][...]
        for ref in part_cols[1:]:
            early = early + ref[...]
        all_ref[...] = jnp.zeros_like(all_ref)
        all_ref[0 : (nb + 1) * rows - rows, :] = early
        all_ref[nb * rows : (nb + 1) * rows, :] = wlast * cols_ref[...]
        by_pair = all_ref[...].T
        sub_t = lax.broadcasted_iota(jnp.int32, (128, 128), 0)
        cell = jnp.where(sub_t < rows, 1.0, 2.0)
        totals = jnp.sum(all_ref[...] * cell, axis=0, keepdims=True)
        sub = lax.broadcasted_iota(jnp.int32, (8, 128), 0)
        lane8 = lax.broadcasted_iota(jnp.int32, (8, 128), 1)
        spot = (lane8 // rows) * 8 + sub
        own = lane8 % rows
        spread = jnp.broadcast_to(totals, (8, 128))

        def shifted(x, by):
            by %= 128
            return pltpu.roll(x, by, 1) if by else x

        q_cross, q_self = pairs // 8, (pairs + 1) // 8
        base = jnp.zeros((8, 128), jnp.float32)
        base = jnp.where((spot == pairs) & (own < pairs), shifted(spread, q_cross * rows), base)
        base = jnp.where((spot == pairs + 1) & (own < la + lb), shifted(spread, q_self * rows - pairs), base)
        for d in range(ndest):
            payload_ref[d] = base
        na = rows_ref.shape[1] // rows
        for j in range(na + nb):
            tile = base
            for q in range(128 // rows):
                if j < na:
                    c0 = j * rows
                    part = shifted(
                        rows_ref[8 * q : 8 * q + 8, c0 // 128 * 128 : c0 // 128 * 128 + 128], q * rows - c0 % 128
                    )
                    if j == 0:
                        part = part + shifted(by_pair[8 * q : 8 * q + 8, :], q * rows)
                else:
                    part = shifted(by_pair[8 * q : 8 * q + 8, :], (q - (j - na + 1)) * rows)
                tile = jnp.where((lane8 // rows == q) & (spot < pairs), part, tile)
            payload_ref[dest_ref[j]] = tile


def last(geo, parts, last_block, nb, totals, dest, weight, ndest):
    la, lb, kt, kv, _, rows, _ = geo
    width = totals.shape[-1]
    na_rows = sum(p[2].shape[1] for p in parts)
    assert (nb + 1) * rows <= 128 and 128 % rows == 0 and na_rows % 128 == 0
    assert 8 * (128 // rows) >= la * lb + 2 and la * lb + la + lb <= 128 and la * lb <= rows
    smem = pl.BlockSpec(memory_space=pltpu.SMEM)
    whole = lambda shape: pl.BlockSpec(shape, lambda i: (0,) * len(shape))
    texts, visions, part_rows, part_cols = zip(*parts)
    return pl.pallas_call(
        lambda *refs: last_kernel(geo, parts, nb, ndest, *refs),
        grid=(max(la, lb),),
        in_specs=[smem, smem, whole(totals.shape)]
        + layer_specs(geo, 1)(width)
        + [pl.BlockSpec((1, *t.shape[1:]), lambda i: (jnp.minimum(i, la - 1), 0, 0)) for t in texts]
        + [pl.BlockSpec((1, *v.shape[1:]), lambda i: (jnp.minimum(i, lb - 1), 0, 0)) for v in visions]
        + [whole(x.shape) for x in (*part_rows, *part_cols)],
        out_specs=whole((ndest, 8, 128)),
        out_shape=jax.ShapeDtypeStruct((ndest, 8, 128), jnp.float32),
        scratch_shapes=[
            pltpu.VMEM((1, rows, kt * width), jnp.bfloat16),
            pltpu.VMEM((1, rows, kv * width), jnp.bfloat16),
            pltpu.VMEM((la, rows, na_rows), jnp.float32),
            pltpu.VMEM((lb, rows, na_rows), jnp.float32),
            pltpu.VMEM((8 * (128 // rows), na_rows), jnp.float32),
            pltpu.VMEM((rows, 128), jnp.float32),
            pltpu.VMEM((128, 128), jnp.float32),
        ],
        compiler_params=pltpu.CompilerParams(vmem_limit_bytes=56 * 1024 * 1024),
        name="last",
    )(dest, weight, totals, last_block, last_block, *texts, *visions, *part_rows, *part_cols)


def finish_kernel(la, lb, rows, count, in_ref, terms_ref, cka_ref):
    pairs = la * lb
    total = jnp.sum(in_ref[...], axis=0)
    spots = jnp.concatenate([total[:, q * rows : (q + 1) * rows] for q in range(128 // rows)], axis=0)
    cross = spots[pairs : pairs + 1, :]
    selves = jnp.broadcast_to(spots[pairs + 1 : pairs + 2, :], (rows, rows)).T
    sub = lax.broadcasted_iota(jnp.int32, (rows, rows), 0)
    lane = lax.broadcasted_iota(jnp.int32, (rows, rows), 1)
    text = jnp.sum(jnp.where(sub == lane // lb, selves, 0.0), axis=0, keepdims=True)
    vision = jnp.sum(jnp.where(sub == la + lane % lb, selves, 0.0), axis=0, keepdims=True)
    inside = lax.broadcasted_iota(jnp.int32, (1, rows), 1) < pairs
    scale = 1.0 / jnp.sqrt(jnp.where(inside, text * vision, 1.0))
    terms = spots.T * (scale * count) if spots.shape[0] == rows else spots.T[:, :rows] * (scale * count)
    terms_ref[...] = terms[:, :pairs]
    cka = cross * scale
    for a in range(la):
        cka_ref[a : a + 1, :] = cka[:, a * lb : (a + 1) * lb]


def finish(received, la, lb, rows, count):
    return pl.pallas_call(
        lambda *refs: finish_kernel(la, lb, rows, count, *refs),
        out_shape=(
            jax.ShapeDtypeStruct((rows, la * lb), jnp.float32),
            jax.ShapeDtypeStruct((la, lb), jnp.float32),
        ),
        name="finish",
    )(received)


def solution(mesh):
    grid = Grid(mesh)
    nx, ny, nz, nc = grid.size
    assert nz % 2 == 0
    ndev = len(grid.at)

    def send(value, shift, senders=None):
        return lax.ppermute(value, AXES, grid.pairs(shift, senders))

    def half_sender(place):
        z = place[2]
        return (z < nz // 2) == ((z % (nz // 2)) % 2 == 0)

    def body(text, vision):
        la, rows, da = text.shape
        lb, _, db = vision.shape
        count = rows * ndev
        width = math.gcd(da, db)
        kt, kv = da // width, db // width
        start = -(-la * kt // kv) * kv
        me = lax.axis_index(AXES)
        own, sums = pack(text, vision, kt, kv, width, start)
        chunks = own.shape[0]

        geo = (la, lb, kt, kv, start, rows, count)
        full_shifts = range(1, (nz + 1) // 2)
        b_blocks = [own] + [send(own, (0, 0, d, 0)) for d in full_shifts]
        b_shifts = [(0, 0, d, 0) for d in full_shifts]

        for k in (3, 0, 1, 2):
            part = sums
            for d in range(1, grid.size[k]):
                shift = tuple(d if i == k else 0 for i in range(4))
                arrived = send(part, shift)
                sums = sums + arrived

        def with_cores(block, dx, dy):
            out = [(block, (dx, dy, 0, 0))]
            for dc in range(1, nc):
                out.append((send(block, (0, 0, 0, dc)), (dx, dy, 0, dc)))
            return out

        plane = {(0, 0): own}
        for d in range(1, nx):
            plane[d, 0] = send(own, (d, 0, 0, 0))
        for d in range(1, ny):
            plane[0, d] = send(own, (0, d, 0, 0))
        early = [pair for (dx, dy), block in plane.items() for pair in with_cores(block, dx, dy)]
        half = chunks // 2
        late = []
        for dx in range(1, nx):
            for dy in range(1, ny):
                first = send(plane[dx, 0][:half], (0, dy, 0, 0))
                second = send(plane[0, dy][half:], (dx, 0, 0, 0))
                late += with_cores(jnp.concatenate([first, second], axis=0), dx, dy)

        weight = np.zeros((ndev,), np.float32)
        last_block = send(own, (0, 0, nz // 2, 0), half_sender)
        b_shifts.append((0, 0, nz // 2, 0))
        for i in range(ndev):
            if half_sender(grid.at[i]):
                weight[grid.moved(i, (0, 0, nz // 2, 0))] = 1.0
        shifts = [s for _, s in early + late] + b_shifts
        table = np.array(
            [[grid.moved(i, tuple(-s for s in shift)) for shift in shifts] for i in range(ndev)], np.int32
        )
        dest = lax.dynamic_index_in_dim(jnp.asarray(table), me, 0, keepdims=False)
        w = lax.dynamic_slice(jnp.asarray(weight), (me,), (1,))
        parts = [region(geo, [x for x, _ in early], b_blocks, sums)]
        if late:
            parts.append(region(geo, [x for x, _ in late], b_blocks, sums))
        payload = last(geo, parts, last_block, len(b_blocks), sums, dest, w, ndev)
        received = lax.all_to_all(payload, AXES, 0, 0, tiled=True)
        return finish(received, la, lb, rows, count)

    spec = P(None, AXES, None)
    return jax.shard_map(body, mesh=mesh, in_specs=(spec, spec), out_specs=(P(AXES, None), P()), check_vma=False)
```
